32 devices in a mesh: chan: 16 (over z, x, core), facet: 2 (over y).
Axes of the slice: x: 2, y: 2, z: 4, core: 2. Of those that a mesh axis runs over, the one named last changes fastest.
Arguments:
- gradients: bfloat16 [64, 4, 1024, 1024], P('chan', None, 'facet'), may hold values from -6 to 6
- taper_map: float32 [1024, 1024], P('facet'), may hold values from 0.1 to 1
- freq_basis: bfloat16 [64, 4], replicated, may hold values from -0.75 to 0.75
- mixing: float32 [4, 4], replicated, may hold values from -3 to 3
- term_model: float32 [16, 1024, 1024], P('chan', 'facet'), may hold values from -6 to 6
Outputs:
- chan_model: bfloat16 [64, 4, 1024, 1024], P('chan', None, 'facet')
- updated: float32 [16, 1024, 1024], P('chan', 'facet')
The draws below stay inside these ranges and needn't reach their ends.
All inputs are finite; a program needn't handle non-finite values.
Results may differ from the reference program's by a relative error of at most 0.0071.
Values may be sent and summed in bfloat16 or wider, within the bound.
A program may use at most 192 MiB of HBM per device.

```python
import math
import jax
import jax.numpy as jnp
from jax import lax

NT = 4
ROWS = 1024
COLS = 1024
FAC = 4
CHANNELS = 64


def shard_levels(stream_key, shape, shards, least, largest):
    gain = 1.0
    for position, blocks in shards:
        heights = jax.random.uniform(jax.random.fold_in(jax.random.fold_in(stream_key, 6), position), (blocks,), jnp.float32, least / len(shards), largest / len(shards))
        gain = gain * jnp.repeat(jnp.exp(heights), shape[position] // blocks).reshape((-1,) + (1,) * (len(shape) - 1 - position))
    return gain


def noise(key, shape, scale, most, pieces=(), kind=jnp.bfloat16):
    array = jax.random.normal(key, shape, jnp.float32) * scale
    if len(pieces) > 0:
        array = shard_levels(key, shape, pieces, -0.22, 0.18) * array
    return jnp.clip(array, min=-most, max=most).astype(kind)


def setup_inputs(seed: int = 0) -> dict:
    key_list = jax.random.split(jax.random.key(seed), 6)
    gradients = noise(key_list[0], (CHANNELS, FAC, ROWS, COLS), 1.0, 6.0, ((0, 16), (2, 2)))
    taper_map = jnp.clip(jnp.exp(math.log(1.0) - 2.3025851 * jax.random.uniform(key_list[1], (ROWS, COLS), jnp.float32) ** shard_levels(key_list[1], (ROWS, COLS), ((0, 2),), -0.2, 0.2)), 0.1, 1.0)
    freq_basis = noise(key_list[2], (CHANNELS, NT), CHANNELS ** -0.5, 0.75)
    mixing = noise(key_list[3], (NT, NT), 0.6, 3.0, (), jnp.float32)
    term_model = noise(key_list[4], (NT * FAC, ROWS, COLS), 1.0, 6.0, ((0, 16), (1, 2)), jnp.float32)
    return {"gradients": gradients, "taper_map": taper_map, "freq_basis": freq_basis, "mixing": mixing, "term_model": term_model}


step_size = 0.3
smooth_weight = 0.2
threshold = 0.5


def reference(gradients, taper_map, freq_basis, mixing, term_model):
    basis_wide = freq_basis.astype(jnp.float32)

    def contract(facet_grads):
        return jnp.einsum('ks,krc->src', basis_wide, facet_grads.astype(jnp.float32))

    contracted = lax.map(contract, jnp.swapaxes(gradients, 0, 1))
    residual_terms = taper_map * jnp.swapaxes(contracted, 0, 1)
    driving = jnp.einsum('ts,sfrc->tfrc', mixing, residual_terms, precision=lax.Precision.HIGHEST)
    current = term_model.reshape(driving.shape)
    padded = jnp.pad(current, ((0, 0), (0, 0), (1, 1), (1, 1)))
    lap = 4.0 * current - padded[:, :, 2:, 1:-1] - padded[:, :, :-2, 1:-1] - padded[:, :, 1:-1, 2:] - padded[:, :, 1:-1, :-2]
    stepped = current + step_size * (driving - smooth_weight * lap)
    updated = stepped - jnp.clip(stepped, -threshold, threshold)
    rounded = updated.astype(jnp.bfloat16)

    def evaluate(facet_terms):
        summed = jnp.einsum('kt,trc->krc', basis_wide, facet_terms.astype(jnp.float32))
        return (taper_map * summed).astype(jnp.bfloat16)

    chan_model = jnp.swapaxes(lax.map(evaluate, jnp.swapaxes(rounded, 0, 1)), 0, 1)
    return chan_model, updated.reshape(term_model.shape)
```

```python
import functools

import jax
import jax.numpy as jnp
from jax import lax
from jax.experimental import pallas as pl
from jax.experimental.pallas import tpu as pltpu
from jax.sharding import PartitionSpec as P

step_size = 0.3
smooth_weight = 0.2
threshold = 0.5
chunks = 2


def extended(cells, axis, dim):
    count = lax.axis_size(axis)
    ends = count - 1
    head = lax.slice_in_dim(cells, 0, 1, axis=dim)
    tail = lax.slice_in_dim(cells, cells.shape[dim] - 1, cells.shape[dim], axis=dim)
    return jnp.concatenate(
        [
            lax.ppermute(tail, axis, [(i, i + 1) for i in range(ends)]),
            cells,
            lax.ppermute(head, axis, [(i + 1, i) for i in range(ends)]),
        ],
        axis=dim,
    )


def laplace(current):
    padded = extended(current.astype(jnp.bfloat16), "facet", 1).astype(current.dtype)
    vertical = padded[:, 2:, :] + padded[:, :-2, :]
    widened = jnp.pad(current, ((0, 0), (0, 0), (1, 1)))
    lateral = widened[:, :, 2:] + widened[:, :, :-2]
    return 4.0 * current - vertical - lateral


def divisor(size, most):
    best = 1
    for candidate in range(1, most + 1):
        if size % candidate == 0:
            best = candidate
    return best


def combine_kernel(tapered, strip, width, weights_ref, images_ref, *refs):
    out_ref = refs[-1]
    outs, ins = out_ref.shape[0], images_ref.shape[0]
    rows, columns = out_ref.shape[2], out_ref.shape[3]

    @pl.loop(0, rows // strip)
    def _(step):
        at = pl.ds(pl.multiple_of(step * strip, strip), strip)
        for left in range(0, columns, width):
            across = pl.ds(left, width)
            cells = [images_ref[i, 0, at, across].astype(jnp.float32) for i in range(ins)]
            taper = refs[0][at, across] if tapered else None
            for o in range(outs):
                total = weights_ref[o, 0] * cells[0]
                for i in range(1, ins):
                    total = total + weights_ref[o, i] * cells[i]
                if tapered:
                    total = total * taper
                out_ref[o, 0, at, across] = total.astype(out_ref.dtype)


def combine(weights, images, taper, out_rows, first_in, first_out, rows, earlier):
    outs, ins = weights.shape
    facets, columns = images.shape[1], images.shape[3]
    tile = divisor(rows, 128)
    strip = divisor(tile, 16)
    width = divisor(columns, 512)
    in_tile, out_tile = first_in // tile, first_out // tile
    operands = [weights, images]
    specs = [
        pl.BlockSpec(memory_space=pltpu.SMEM),
        pl.BlockSpec((ins, 1, tile, columns), lambda r, f: (0, f, in_tile + r, 0)),
    ]
    if taper is not None:
        operands.append(taper)
        specs.append(pl.BlockSpec((tile, columns), lambda r, f: (out_tile + r, 0)))
    aliases = {}
    if earlier is not None:
        aliases = {len(operands): 0}
        operands.append(earlier)
        specs.append(pl.BlockSpec(memory_space=pl.ANY))
    pixels = facets * rows * columns
    return pl.pallas_call(
        functools.partial(combine_kernel, taper is not None, strip, width),
        out_shape=jax.ShapeDtypeStruct((outs, facets, out_rows, columns), jnp.bfloat16),
        grid=(rows // tile, facets),
        in_specs=specs,
        out_specs=pl.BlockSpec((outs, 1, tile, columns), lambda r, f: (0, f, out_tile + r, 0)),
        input_output_aliases=aliases,
        cost_estimate=pl.CostEstimate(
            flops=2 * outs * ins * pixels, bytes_accessed=2 * (outs + ins) * pixels, transcendentals=0
        ),
    )(*operands)


def on_device(gradients, taper_map, freq_basis, mixing, term_model):
    local_chans, facets, band_rows, columns = gradients.shape
    term_count = freq_basis.shape[1]
    own_basis = lax.dynamic_slice_in_dim(
        freq_basis, lax.axis_index("chan") * local_chans, local_chans, 0
    ).astype(jnp.float32)
    weights = jnp.sum(mixing[:, None, :] * own_basis[None, :, :], axis=2)
    smoothed = term_model - (step_size * smooth_weight) * laplace(term_model)
    rows = band_rows // chunks
    summed = []
    for chunk in range(chunks):
        driving = combine(weights, gradients, None, rows, chunk * rows, 0, rows, None)
        flat = driving.reshape(term_count * facets, rows, columns)
        summed.append(lax.psum_scatter(flat, "chan", scatter_dimension=0, tiled=True))
    pieces = []
    chan_model = None
    for chunk in range(chunks):
        at = chunk * rows
        taper = taper_map[at : at + rows]
        stepped = smoothed[:, at : at + rows] + step_size * (
            taper * summed[chunk].astype(jnp.float32)
        )
        updated = stepped - jnp.clip(stepped, -threshold, threshold)
        pieces.append(updated)
        slabs = lax.all_gather(updated.astype(jnp.bfloat16), "chan", axis=0, tiled=True)
        terms = slabs.reshape(term_count, facets, rows, columns)
        chan_model = combine(own_basis, terms, taper_map, band_rows, 0, at, rows, chan_model)
    updated = pieces[0] if chunks == 1 else jnp.concatenate(pieces, axis=1)
    return (chan_model, updated)


def solution(mesh):
    return jax.shard_map(
        on_device,
        mesh=mesh,
        in_specs=(
            P("chan", None, "facet", None),
            P("facet", None),
            P(),
            P(),
            P("chan", "facet", None),
        ),
        out_specs=(P("chan", None, "facet", None), P("chan", "facet", None)),
        check_vma=False,
    )
```
